8 devices in a mesh: rep: 1 (over z), pp: 8 (over x, y, core).
Axes of the slice: x: 2, y: 2, z: 1, core: 2. Of those that a mesh axis runs over, the one named last changes fastest.
Arguments:
- x: bfloat16 [16, 512, 512], P('rep')
- dy: bfloat16 [16, 512, 512], P('rep')
- w_gate: bfloat16 [8, 512, 1664], P('pp')
- w_up: bfloat16 [8, 512, 1664], P('pp')
- w_down: bfloat16 [8, 1664, 512], P('pp')
Outputs:
- output 1: bfloat16 [8, 512, 1664], P(('rep', 'pp'))
- output 2: bfloat16 [8, 512, 1664], P(('rep', 'pp'))
- output 3: bfloat16 [8, 1664, 512], P(('rep', 'pp'))
All inputs are finite; a program needn't handle non-finite values.
Results may differ from the reference program's by a relative error of at most 0.0274.
Values are sent between devices in bfloat16 or wider.
A program may use at most 2 GiB of HBM per device.

```python
import jax
import jax.numpy as jnp
from jax import lax

MICRO = 16
TOKENS = 512
D = 512
FF = 1664
LAYERS = 8
NAMES = ("w_gate", "w_up", "w_down")
SHAPES = {"w_gate": (LAYERS, D, FF), "w_up": (LAYERS, D, FF), "w_down": (LAYERS, FF, D)}


def bump(key, n, height):
    away = (jnp.arange(n, dtype=jnp.int32) - jax.random.randint(key, (), 0, n, jnp.int32)) % n
    return jnp.where(away < n // 8, height, 1.0)


def together(key, own, strength):
    shared = jax.random.normal(key, own.shape[1:], jnp.float32)
    return (own + strength * shared) * lax.rsqrt(1 + strength * strength)


def setup_inputs(seed: int = 0, part: int = 0) -> dict:
    kx, kdy, ka, kb, kz, kf, kh, kl, *kw = jax.random.split(jax.random.key(seed), 8 + len(NAMES))
    kx, kdy, ka, kb = (jax.random.fold_in(k, part) for k in (kx, kdy, ka, kb))
    shape = (MICRO, TOKENS, D)
    much_x, much_dy = jax.random.uniform(kz, (2,), jnp.float32, 0.0, 1.0)
    layers = 2.0 ** jax.random.uniform(kl, (LAYERS, 1, 1), jnp.float32, -1.0, 1.0)
    x = together(ka, jax.random.normal(kx, shape, jnp.float32), much_x) * bump(kf, D, 4.0)
    dy = together(kb, jax.random.normal(kdy, shape, jnp.float32), much_dy)
    drawn = {"x": x.astype(jnp.bfloat16), "dy": (dy * (MICRO * TOKENS) ** -0.5).astype(jnp.bfloat16)}
    for key, name in zip(kw, NAMES, strict=True):
        w = jax.random.normal(key, SHAPES[name], jnp.float32) * SHAPES[name][1] ** -0.5
        drawn[name] = (w * {"w_gate": 1.0, "w_up": bump(kh, FF, 4.0), "w_down": layers}[name]).astype(jnp.bfloat16)
    return drawn


def matmul(a, w):
    return jnp.dot(a, w, preferred_element_type=jnp.float32).astype(jnp.bfloat16)


def normed(h):
    wide = h.astype(jnp.float32)
    scale = lax.rsqrt(jnp.mean(wide**2, -1, keepdims=True) + 1e-6)
    return (wide * scale).astype(jnp.bfloat16)


def layer(h, w):
    a = normed(h)
    gate = jnp.dot(a, w["w_gate"], preferred_element_type=jnp.float32)
    up = jnp.dot(a, w["w_up"], preferred_element_type=jnp.float32)
    return h + matmul((jax.nn.silu(gate) * up).astype(jnp.bfloat16), w["w_down"])


def stack(weights, h):
    return lax.scan(lambda h, w: (layer(h, w), None), h, weights)[0]


def reference(x, dy, w_gate, w_up, w_down):
    weights = dict(zip(NAMES, (w_gate, w_up, w_down), strict=True))

    def take(so_far, one):
        h, by_y = one
        _, back = jax.vjp(lambda w: stack(w, h), weights)
        return jax.tree.map(lambda total, term: total + term.astype(jnp.float32), so_far, back(by_y)[0]), None

    none_yet = {name: jnp.zeros(w.shape, jnp.float32) for name, w in weights.items()}
    by_weights, _ = lax.scan(take, none_yet, (x, dy))
    return tuple(by_weights[name].astype(jnp.bfloat16) for name in NAMES)
```

```python
import jax
import jax.numpy as jnp
from jax import lax
from jax.experimental import pallas as pl
from jax.experimental.pallas import tpu as pltpu
from jax.sharding import PartitionSpec as P

F32, BF16 = jnp.float32, jnp.bfloat16
MICRO, T, D, FF, STAGES = 16, 512, 512, 1664, 8
PARTS = 2
C = T // PARTS
CHUNKS = MICRO * PARTS
BLOCKS = FF // 128
RING = 4
SLOTS = 4
AHEAD = (24, 19, 16, 13, 9, 6, 2, 0)
LATE = (0, 1, 2, 0, 3, 3, 3, 3)


def dot(a, b):
    return jnp.dot(a, b, preferred_element_type=F32)


def dot_rows(a, b):
    return lax.dot_general(a, b, (((0,), (0,)), ((), ())), preferred_element_type=F32)


def sigmoid(x):
    return 0.5 * jnp.tanh(0.5 * x) + 0.5


def scale_of(wide):
    return lax.rsqrt(jnp.mean(wide * wide, -1, keepdims=True) + 1e-6)


def forward(h, wgu, wd, act):
    wide = h.astype(F32)
    a = (wide * scale_of(wide)).astype(BF16)
    for j in range(BLOCKS):
        both = dot(a, wgu[:, 256 * j : 256 * j + 256])
        gate, up = both[:, :128], both[:, 128:]
        act[:, 128 * j : 128 * j + 128] = (gate * sigmoid(gate) * up).astype(BF16)
    return h + dot(act[...], wd[...]).astype(BF16)


def backward(h, dy, wgu, wdt, wgut, act, dgu, further):
    wide = h.astype(F32)
    scale = scale_of(wide)
    a = (wide * scale).astype(BF16)
    for start in range(0, BLOCKS, 2):
        blocks = range(start, min(start + 2, BLOCKS))
        by_act = dot(dy, wdt[:, 128 * start : 128 * blocks[-1] + 128]).astype(BF16).astype(F32)
        for j in blocks:
            both = dot(a, wgu[:, 256 * j : 256 * j + 256])
            gate, up = both[:, :128], both[:, 128:]
            by = by_act[:, 128 * (j - start) : 128 * (j - start) + 128]
            s = sigmoid(gate)
            silu = gate * s
            act[:, 128 * j : 128 * j + 128] = (silu * up).astype(BF16)
            dgu[:, 256 * j : 256 * j + 128] = (by * up * (s + silu * (1.0 - s))).astype(BF16)
            dgu[:, 256 * j + 128 : 256 * j + 256] = (by * silu).astype(BF16)
    if not further:
        return None
    by_a = dot(dgu[...], wgut[...]).astype(BF16).astype(F32)
    by_scale = jnp.sum(by_a * wide, -1, keepdims=True)
    by_wide = by_a * scale - wide * (by_scale * scale * scale * scale * (1.0 / D))
    return dy + by_wide.astype(BF16)


def by_weights(h, dy, act, dgu, sum_gu, sum_d):
    wide = h.astype(F32)
    at = (wide * scale_of(wide)).astype(BF16).T
    for j in range(BLOCKS):
        at_j = slice(256 * j, 256 * j + 256)
        sum_gu[:, at_j] += dot(at, dgu[:, at_j]).astype(BF16).astype(F32)
    for start in range(0, FF, 256):
        rows = slice(start, min(start + 256, FF))
        sum_d[rows, :] += dot_rows(act[:, rows], dy).astype(BF16).astype(F32)


def pick(me, values):
    return sum(jnp.where(me == i, v, 0) for i, v in enumerate(values))


def kernel(x, dy, wg_in, wu_in, wd_in, dwg, dwu, dwd, hs, dys, wgu, wd, wdt, wgut, sum_gu, sum_d, act_f, act, dgu, out_f, out_b,
           got_f, got_b, sent_f, sent_b, loaded, stored):
    me = lax.axis_index("pp")
    after, before = lax.rem(me + 1, STAGES), lax.rem(me + STAGES - 1, STAGES)
    first, last = me == 0, me == STAGES - 1
    ahead, late = pick(me, AHEAD), pick(me, LATE)

    def rows(c):
        return pl.ds(pl.multiple_of(c * C, C), C)

    loads = []
    for j in range(BLOCKS):
        loads.append(pltpu.make_async_copy(wg_in.at[0, :, pl.ds(128 * j, 128)], wgu.at[:, pl.ds(256 * j, 128)], loaded.at[2 * j]))
        loads.append(pltpu.make_async_copy(wu_in.at[0, :, pl.ds(128 * j, 128)], wgu.at[:, pl.ds(256 * j + 128, 128)], loaded.at[2 * j + 1]))
    loads.append(pltpu.make_async_copy(wd_in.at[0], wd, loaded.at[2 * BLOCKS]))
    for load in loads:
        load.start()

    def local_f(c):
        return pltpu.make_async_copy(x.at[c // PARTS, pl.ds(pl.multiple_of(lax.rem(c, PARTS) * C, C), C), :], hs.at[rows(c), :], got_f.at[c])

    def local_b(c):
        return pltpu.make_async_copy(dy.at[c // PARTS, pl.ds(pl.multiple_of(lax.rem(c, PARTS) * C, C), C), :], dys.at[rows(c), :], got_b.at[c])

    @pl.when(first)
    def _():
        lax.fori_loop(0, CHUNKS, lambda c, n: (local_f(c).start(), n)[1], 0)

    @pl.when(last)
    def _():
        lax.fori_loop(0, CHUNKS, lambda c, n: (local_b(c).start(), n)[1], 0)

    def send_f(c):
        slot = lax.rem(c, RING)
        return pltpu.make_async_remote_copy(out_f.at[slot], hs.at[rows(c), :], sent_f.at[slot], got_f.at[c],
                                            device_id={"pp": after}, device_id_type=pl.DeviceIdType.MESH)

    def send_b(c):
        slot = lax.rem(c, RING)
        return pltpu.make_async_remote_copy(out_b.at[slot], dys.at[rows(c), :], sent_b.at[slot], got_b.at[c],
                                            device_id={"pp": before}, device_id_type=pl.DeviceIdType.MESH)

    barrier = pltpu.get_barrier_semaphore()

    @pl.when(jnp.logical_not(last))
    def _():
        pl.semaphore_signal(barrier, inc=1, device_id={"pp": after}, device_id_type=pl.DeviceIdType.MESH)

    @pl.when(jnp.logical_not(first))
    def _():
        pl.semaphore_signal(barrier, inc=1, device_id={"pp": before}, device_id_type=pl.DeviceIdType.MESH)

    pl.semaphore_wait(barrier, jnp.where(first | last, 1, 2))
    for load in loads:
        load.wait()

    def step(t, carry):
        @pl.when(t == jnp.where(first, 8, 0))
        def _():
            for j in range(BLOCKS):
                wgut[256 * j : 256 * j + 256, :] = wgu[:, 256 * j : 256 * j + 256].T
            for start in range(0, FF, 256):
                at_s = slice(start, min(start + 256, FF))
                wdt[:, at_s] = wd[at_s, :].T
            sum_gu[...] = jnp.zeros_like(sum_gu)
            sum_d[...] = jnp.zeros_like(sum_d)

        @pl.when((t < CHUNKS) & jnp.logical_not(last))
        def _():
            local_f(t).wait()

            @pl.when(t >= RING)
            def _():
                send_f(t - RING).wait_send()

            out_f[lax.rem(t, RING)] = forward(hs[rows(t), :], wgu, wd, act_f)
            send_f(t).start()

        c = t - ahead

        @pl.when((c >= 0) & (c < CHUNKS))
        def _():
            slot, part = lax.rem(c // PARTS, SLOTS), rows(lax.rem(c, PARTS))
            local_b(c).wait()
            act_c, dgu_c = act.at[slot, part, :], dgu.at[slot, part, :]

            @pl.when(first)
            def _():
                backward(hs[rows(c), :], dys[rows(c), :], wgu, wdt, wgut, act_c, dgu_c, False)

            @pl.when(last)
            def _():
                local_f(c).wait()

            @pl.when(jnp.logical_not(first))
            def _():
                @pl.when(c >= RING)
                def _():
                    send_b(c - RING).wait_send()

                out_b[lax.rem(c, RING)] = backward(hs[rows(c), :], dys[rows(c), :], wgu, wdt, wgut, act_c, dgu_c, True)
                send_b(c).start()

        m = c // PARTS - late

        @pl.when((c >= 0) & (lax.rem(c, PARTS) == PARTS - 1) & (m >= 0) & (m < MICRO))
        def _():
            slot, part = lax.rem(m, SLOTS), pl.ds(pl.multiple_of(m * T, T), T)
            by_weights(hs[part, :], dys[part, :], act.at[slot], dgu.at[slot], sum_gu, sum_d)

        return carry

    lax.fori_loop(0, CHUNKS + ahead + late * PARTS, step, 0)

    @pl.when(jnp.logical_not(last))
    def _():
        lax.fori_loop(CHUNKS - RING, CHUNKS, lambda c, n: (send_f(c).wait_send(), n)[1], 0)

    @pl.when(jnp.logical_not(first))
    def _():
        lax.fori_loop(CHUNKS - RING, CHUNKS, lambda c, n: (send_b(c).wait_send(), n)[1], 0)

    stores = []
    for j in range(BLOCKS):
        cols = slice(256 * j, 256 * j + 256)
        dgu[0, :, cols] = sum_gu[:, cols].astype(BF16)
        stores.append(pltpu.make_async_copy(dgu.at[0, :, pl.ds(256 * j, 128)], dwg.at[0, :, pl.ds(128 * j, 128)], stored.at[2 * j]))
        stores.append(pltpu.make_async_copy(dgu.at[0, :, pl.ds(256 * j + 128, 128)], dwu.at[0, :, pl.ds(128 * j, 128)], stored.at[2 * j + 1]))
        stores[-2].start()
        stores[-1].start()
    wd[...] = sum_d[...].astype(BF16)
    stores.append(pltpu.make_async_copy(wd, dwd.at[0], stored.at[2 * BLOCKS]))
    stores[-1].start()
    for store in stores:
        store.wait()


def solution(mesh):
    def step(x, dy, w_gate, w_up, w_down):
        v, sem = pltpu.VMEM, pltpu.SemaphoreType.DMA
        return pl.pallas_call(
            kernel,
            out_shape=[jax.ShapeDtypeStruct(w.shape, w.dtype) for w in (w_gate, w_up, w_down)],
            in_specs=[pl.BlockSpec(memory_space=pl.ANY)] * 5,
            out_specs=[pl.BlockSpec(memory_space=pl.ANY)] * 3,
            scratch_shapes=[
                v((MICRO * T, D), BF16), v((MICRO * T, D), BF16),
                v((D, 2 * FF), BF16), v((FF, D), BF16), v((D, FF), BF16), v((2 * FF, D), BF16),
                v((D, 2 * FF), F32), v((FF, D), F32),
                v((C, FF), BF16), v((SLOTS, T, FF), BF16), v((SLOTS, T, 2 * FF), BF16),
                v((RING, C, D), BF16), v((RING, C, D), BF16),
                sem((CHUNKS,)), sem((CHUNKS,)), sem((RING,)), sem((RING,)), sem((2 * BLOCKS + 1,)), sem((2 * BLOCKS + 1,)),
            ],
            compiler_params=pltpu.CompilerParams(collective_id=0, has_side_effects=True, vmem_limit_bytes=67043328),
        )(x, dy, w_gate, w_up, w_down)

    return jax.shard_map(
        step,
        mesh=mesh,
        in_specs=(P("rep", None, None),) * 2 + (P("pp", None, None),) * 3,
        out_specs=(P(("rep", "pp"), None, None),) * 3,
        check_vma=False,
    )
```

```python
import jax
import jax.numpy as jnp
from jax import lax
from jax.experimental import pallas as pl
from jax.experimental.pallas import tpu as pltpu
from jax.sharding import PartitionSpec as P

F32, BF16 = jnp.float32, jnp.bfloat16
MESH = pl.DeviceIdType.MESH
MICRO, T, D, FF, STAGES = 16, 512, 512, 1664, 8
LAST = STAGES - 1
BLOCKS = FF // 128
LARGE, SMALL = 256, 128
HEAD, TAIL = 1, 1
RING = 4
SLOTS = 3
DEPTH = 6
OVER_F, OVER_B = range(1, 15), range(0)
ORDER = (
    (0x181911911111111111111, 0x12512A831191111A93A19, 0x1622624622C25A235A22C, 0x1626222626622624),
    (0x113311111111111111111, 0x152251113263137112311, 0x162626262626626224522, 0x14622222),
    (0x113311313111111111111, 0x125225326353252531253, 0x122222622262625226353, 0x1446),
    (0x131513313311111111111, 0x152523235227347331253, 0x144622222626263266312),
    (0x131271315331131311111, 0x125232522526316331635, 0x144622226272312737),
    (0x131522713111533331111, 0x172735232631573266313, 0x144622273272312),
    (0x133723512317137223111, 0x172352337527336371316, 0x144622317132),
    (0x166222622622466222222, 0x16224622622266224662),
)
WORD = 7
INIT_AT = 8

PIECES = MICRO * T // 128
TAIL_AT = PIECES - 4 * TAIL
CHUNKS = 4 * HEAD + 2 * (MICRO - HEAD - TAIL) + 4 * TAIL


def steps(numbers):
    digits = []
    for number in numbers:
        while number > 1:
            digits.append(number % 16)
            number //= 16
    return digits


def words(numbers, count):
    digits = steps(numbers)
    digits += [0] * (WORD * count - len(digits))
    return [sum(d * 16**i for i, d in enumerate(digits[at : at + WORD])) for at in range(0, WORD * count, WORD)]


def piece(k):
    middle, tail = 4 * HEAD, CHUNKS - 4 * TAIL
    return jnp.where(k < middle, k, jnp.where(k < tail, middle + 2 * (k - middle), TAIL_AT + k - tail))


def is_small(p):
    return (p < 4 * HEAD) | (p >= TAIL_AT)


def dot(a, b):
    return jnp.dot(a, b, preferred_element_type=F32)


def dot_rows(a, b):
    return lax.dot_general(a, b, (((0,), (0,)), ((), ())), preferred_element_type=F32)


def sigmoid(x):
    return 0.5 * jnp.tanh(0.5 * x) + 0.5


def scale_of(wide):
    return lax.rsqrt(jnp.mean(wide * wide, -1, keepdims=True) + 1e-6)


def hidden(a, j, wgu):
    both = dot(a, wgu[:, 256 * j : 256 * j + 256])
    gate, up = both[:, :128], both[:, 128:]
    s = sigmoid(gate)
    silu = gate * s
    return silu, up * (s + silu * (1.0 - s)), (silu * up).astype(BF16)


def forward(h, wgu, wd, act, kept):
    wide = h.astype(F32)
    a = (wide * scale_of(wide)).astype(BF16)
    for j in range(BLOCKS):
        silu, slope, act[:, 128 * j : 128 * j + 128] = hidden(a, j, wgu)
        kept[:, 256 * j : 256 * j + 128] = slope
        kept[:, 256 * j + 128 : 256 * j + 256] = silu
    return h + dot(act[...], wd[...]).astype(BF16)


def backward(h, dy, wgu, wdt, wgut, act, dgu, kept, further):
    wide = h.astype(F32)
    scale = scale_of(wide)
    if kept is None:
        a = (wide * scale).astype(BF16)
    for start in range(0, BLOCKS, 2):
        blocks = range(start, min(start + 2, BLOCKS))
        by_act = dot(dy, wdt[:, 128 * start : 128 * blocks[-1] + 128]).astype(BF16).astype(F32)
        for j in blocks:
            by = by_act[:, 128 * (j - start) : 128 * (j - start) + 128]
            if kept is None:
                silu, slope, act[:, 128 * j : 128 * j + 128] = hidden(a, j, wgu)
            else:
                slope, silu = kept[:, 256 * j : 256 * j + 128], kept[:, 256 * j + 128 : 256 * j + 256]
            dgu[:, 256 * j : 256 * j + 128] = (by * slope).astype(BF16)
            dgu[:, 256 * j + 128 : 256 * j + 256] = (by * silu).astype(BF16)
    if not further:
        return None
    by_a = dot(dgu[...], wgut[...]).astype(BF16).astype(F32)
    by_scale = jnp.sum(by_a * wide, -1, keepdims=True)
    by_wide = by_a * scale - wide * (by_scale * scale * scale * scale * (1.0 / D))
    return dy + by_wide.astype(BF16)


def by_weights(h, dy, act, dgu, sum_gu, sum_d):
    wide = h.astype(F32)
    at = (wide * scale_of(wide)).astype(BF16).T
    for j in range(BLOCKS):
        at_j = slice(256 * j, 256 * j + 256)
        sum_gu[:, at_j] += dot(at, dgu[:, at_j]).astype(BF16).astype(F32)
    for start in range(0, FF, 256):
        rows = slice(start, min(start + 256, FF))
        sum_d[rows, :] += dot_rows(act[:, rows], dy).astype(BF16).astype(F32)


def pick(me, values):
    return sum(jnp.where(me == i, v, 0) for i, v in enumerate(values))


def kernel(x, dy, wg_in, wu_in, wd_in, dwg, dwu, dwd, kept_far, act_far, hs, dys, wgu, wd, wdt, wgut, sum_gu, sum_d, act_f, kept_f, kept_b,
           act, dgu, out_f, out_b, got_f, got_b, got_pass, sent_f, sent_b, sent_pass, saved, loaded, brought, stored, credit, room):
    me = lax.axis_index("pp")
    after, before = lax.rem(me + 1, STAGES), lax.rem(me + LAST, STAGES)
    first, last = me == 0, me == LAST

    def tokens(ref, p, n):
        return ref.at[p // 4, pl.ds(pl.multiple_of(lax.rem(p, 4) * 128, 128), n), :]

    def rows(p, n):
        return pl.ds(pl.multiple_of(p * 128, 128), n)

    def ring(p, n):
        return rows(lax.rem(p, 2 * RING), n)

    def deep(p, n):
        return rows(lax.rem(p, 4 * DEPTH), n)

    def whole(ref, m):
        return ref.at[rows(lax.rem(m, RING) * 2, LARGE), :]

    fetch = []
    for j in range(BLOCKS):
        fetch.append(pltpu.make_async_copy(wg_in.at[0, :, pl.ds(128 * j, 128)], wgu.at[:, pl.ds(256 * j, 128)], brought.at[2 * j]))
        fetch.append(pltpu.make_async_copy(wu_in.at[0, :, pl.ds(128 * j, 128)], wgu.at[:, pl.ds(256 * j + 128, 128)], brought.at[2 * j + 1]))
    fetch.append(pltpu.make_async_copy(wd_in.at[0], wd, brought.at[2 * BLOCKS]))
    for copy in fetch:
        copy.start()

    def local_f(p, n):
        return pltpu.make_async_copy(tokens(x, p, n), hs.at[rows(p, n), :], got_f.at[p])

    def local_b(p, n):
        return pltpu.make_async_copy(tokens(dy, p, n), dys.at[deep(p, n), :], got_b.at[p])

    def chunks(m):
        n = SMALL if m < HEAD or m >= MICRO - TAIL else LARGE
        return [(4 * m + r // 128, n) for r in range(0, T, n)]

    @pl.when(first)
    def _():
        for m in range(MICRO):
            for chunk in chunks(m):
                local_f(*chunk).start()

    @pl.when(last)
    def _():
        for m in range(DEPTH):
            for chunk in chunks(m):
                local_b(*chunk).start()

    barrier = pltpu.get_barrier_semaphore()
    links = [{i - 1, i + 1} & set(range(STAGES)) for i in range(STAGES)]
    for i, j in ((0, 3), (0, 4), (7, 4), (7, 3)):
        links[i].add(j)
        links[j].add(i)
    for i in range(STAGES):

        @pl.when(me == i)
        def _(i=i):
            for j in sorted(links[i]):
                pl.semaphore_signal(barrier, inc=1, device_id={"pp": j}, device_id_type=MESH)

    pl.semaphore_wait(barrier, pick(me, [len(link) for link in links]))
    for copy in fetch:
        copy.wait()

    def send(source, target, sent, got, device):
        return pltpu.make_async_remote_copy(source, target, sent, got, device_id={"pp": device}, device_id_type=MESH)

    def send_f(p, n):
        return send(out_f.at[ring(p, n), :], hs.at[rows(p, n), :], sent_f.at[lax.rem(p, 2 * RING)], got_f.at[p], after)

    def send_b(p, n):
        return send(out_b.at[ring(p, n), :], dys.at[deep(p, n), :], sent_b.at[lax.rem(p, 2 * RING)], got_b.at[p], before)

    def over_f(p):
        return send(out_f.at[ring(p, LARGE), :], whole(out_b, p // 4), sent_f.at[lax.rem(p, 2 * RING)], got_pass.at[lax.rem(p // 4, RING)], 0)

    def over_b(p):
        return send(out_b.at[ring(p, LARGE), :], whole(out_f, p // 4), sent_b.at[lax.rem(p, 2 * RING)], got_pass.at[lax.rem(p // 4, RING)], LAST)

    def pass_f(m):
        p = 4 * m + 2
        return send(whole(out_b, m), hs.at[rows(p, LARGE), :], sent_pass.at[lax.rem(m, RING)], got_f.at[p], 4)

    def pass_b(m):
        p = 4 * m + 2
        return send(whole(out_f, m), dys.at[deep(p, LARGE), :], sent_pass.at[lax.rem(m, RING)], got_b.at[p], 3)

    def saves(k, p, n):
        buffer = lax.rem(k, 2)
        return (pltpu.make_async_copy(kept_f.at[buffer, pl.ds(0, n), :], kept_far.at[rows(p, n), :], saved.at[2 * buffer]),
                pltpu.make_async_copy(act_f.at[buffer, pl.ds(0, n), :], act_far.at[rows(p, n), :], saved.at[2 * buffer + 1]))

    def loads(k, p, n):
        buffer, slot, part = lax.rem(k, 2), lax.rem(p // 4, SLOTS), rows(lax.rem(p, 4), n)
        return (pltpu.make_async_copy(kept_far.at[rows(p, n), :], kept_b.at[buffer, pl.ds(0, n), :], loaded.at[2 * buffer]),
                pltpu.make_async_copy(act_far.at[rows(p, n), :], act.at[slot, part, :], loaded.at[2 * buffer + 1]))

    def each_size(condition, p, do):
        for n in (LARGE, SMALL):

            @pl.when(condition & (is_small(p) if n == SMALL else jnp.logical_not(is_small(p))))
            def _(n=n):
                do(n)

    def wait_saved(condition, k):
        p = piece(k)

        def do(n):
            for copy in saves(k, p, n):
                copy.wait()

        each_size(condition, p, do)

    def load(condition, k, have_saved):
        p = piece(k)
        with jax.named_scope("saved"):
            wait_saved(condition & (have_saved <= k), k)

        def do(n):
            for copy in loads(k, p, n):
                copy.start()

        each_size(condition, p, do)
        return jnp.where(condition, jnp.maximum(have_saved, k + 1), have_saved)

    def free_ring(copy, p, n):
        if n == LARGE:

            @pl.when((p >= 2 * RING) & (p < 2 * RING + 4 * HEAD))
            def _():
                copy(p - 2 * RING, SMALL).wait_send()
                copy(p - 2 * RING + 1, SMALL).wait_send()

            @pl.when(p >= 2 * RING + 4 * HEAD)
            def _():
                copy(p - 2 * RING, LARGE).wait_send()
        else:

            @pl.when((p >= TAIL_AT) & (lax.rem(p, 2) == 0))
            def _():
                copy(p - 2 * RING, LARGE).wait_send()

    def inside(m, over):
        return (m >= over.start) & (m < over.stop)

    def passed(condition, m):
        with jax.named_scope("passed"):

            @pl.when(condition)
            def _():
                pass_f(m).wait_send()

            @pl.when(condition & first & inside(m + RING, OVER_F))
            def _():
                pl.semaphore_signal(credit, inc=1, device_id={"pp": 3}, device_id_type=MESH)

            @pl.when(condition & last & inside(m + RING, OVER_B))
            def _():
                pl.semaphore_signal(credit, inc=1, device_id={"pp": 4}, device_id_type=MESH)

    def take_forward(k, p, n, have_saved):
        with jax.named_scope("f_wait"):
            local_f(p, n).wait()
        with jax.named_scope("f_free"):
            free_ring(send_f, p, n)
            wait_saved((k >= 2) & (have_saved <= k - 2), k - 2)
        with jax.named_scope("f"):
            buffer = lax.rem(k, 2)
            out_f[ring(p, n), :] = forward(hs[rows(p, n), :], wgu, wd, act_f.at[buffer, pl.ds(0, n), :], kept_f.at[buffer, pl.ds(0, n), :])
            via = jnp.bool_(False)
            if n == LARGE and len(OVER_F):
                m = p // 4
                via = (me == 3) & (lax.rem(p, 4) == 2) & inside(m, OVER_F)

                @pl.when(via & (m >= OVER_F.start + RING))
                def _():
                    pl.semaphore_wait(credit, 1)

                @pl.when(via)
                def _():
                    over_f(p).start()

            @pl.when(jnp.logical_not(via))
            def _():
                send_f(p, n).start()

            for copy in saves(k, p, n):
                copy.start()

    def take_backward(k, p, n):
        m, part = p // 4, rows(lax.rem(p, 4), n)
        slot, buffer = lax.rem(m, SLOTS), lax.rem(k, 2)
        act_c, dgu_c, kept = act.at[slot, part, :], dgu.at[slot, part, :], kept_b.at[buffer, pl.ds(0, n), :]
        with jax.named_scope("b"):
            h, by = hs.at[rows(p, n), :], dys.at[deep(p, n), :]

            @pl.when(first)
            def _():
                backward(h[...], by[...], wgu, wdt, wgut, act_c, dgu_c, kept, False)

            @pl.when(jnp.logical_not(first))
            def _():
                @pl.when((m >= DEPTH) & (lax.rem(p, 4) == 0))
                def _():
                    pl.semaphore_wait(room, 1)

                free_ring(send_b, p, n)

            @pl.when(last)
            def _():
                out_b[ring(p, n), :] = backward(h[...], by[...], wgu, wdt, wgut, act_c, dgu_c, None, True)

            @pl.when(jnp.logical_not(first | last))
            def _():
                out_b[ring(p, n), :] = backward(h[...], by[...], wgu, wdt, wgut, act_c, dgu_c, kept, True)

            via = jnp.bool_(False)
            if n == LARGE and len(OVER_B):
                via = (me == 4) & (lax.rem(p, 4) == 2) & inside(m, OVER_B)

                @pl.when(via & (m >= OVER_B.start + RING))
                def _():
                    pl.semaphore_wait(credit, 1)

                @pl.when(via)
                def _():
                    over_b(p).start()

            @pl.when(jnp.logical_not(first | via))
            def _():
                send_b(p, n).start()

    def take_weights(m):
        slot, part = lax.rem(m, SLOTS), pl.ds(pl.multiple_of(m * T, T), T)
        by_weights(hs[part, :], dys[deep(4 * m, T), :], act.at[slot], dgu.at[slot], sum_gu, sum_d)

        @pl.when((m < MICRO - DEPTH) & jnp.logical_not(last))
        def _():
            pl.semaphore_signal(room, inc=1, device_id={"pp": after}, device_id_type=MESH)

        for later in range(DEPTH, MICRO):

            @pl.when(last & (m == later - DEPTH))
            def _(later=later):
                for chunk in chunks(later):
                    local_b(*chunk).start()

    def prepare():
        with jax.named_scope("init"):
            for j in range(BLOCKS):
                wgut[256 * j : 256 * j + 256, :] = wgu[:, 256 * j : 256 * j + 256].T
            for start in range(0, FF, 256):
                at_s = slice(start, min(start + 256, FF))
                wdt[:, at_s] = wd[at_s, :].T
            sum_gu[...] = jnp.zeros_like(sum_gu)
            sum_d[...] = jnp.zeros_like(sum_d)

    def step(s, carry):
        digits, n_f, n_b, n_w, n_p, n_saved, n_loaded = carry
        digit, digits = lax.rem(digits, 16), digits // 16
        do_f, do_b, do_w, do_p = (lax.rem(digit // d, 2) for d in (1, 2, 4, 8))
        keeps = jnp.logical_not(last)

        @pl.when(s == jnp.where(first, INIT_AT, 0))
        def _():
            prepare()

        if len(OVER_F) or len(OVER_B):
            begin = jnp.where(first, OVER_F.start, OVER_B.start)

            @pl.when(do_p == 1)
            def _():
                m = begin + n_p
                passed(n_p > 0, m - 1)
                with jax.named_scope("pass"):
                    pltpu.make_async_copy(tokens(x, 4 * m, LARGE), whole(out_b, m), got_pass.at[lax.rem(m, RING)]).wait()

                    @pl.when(first)
                    def _():
                        pass_f(m).start()

                    @pl.when(last)
                    def _():
                        pass_b(m).start()

        p = piece(n_f)
        each_size(do_f == 1, p, lambda n: take_forward(n_f, p, n, n_saved))
        n_saved = jnp.where((do_f == 1) & (n_f >= 2), jnp.maximum(n_saved, n_f - 1), n_saved)
        n_f += do_f

        def can_load(known):
            return keeps & (n_loaded < known) & (n_loaded < n_b + 2) & (n_w > piece(n_loaded) // 4 - SLOTS)

        early = (do_f == 1) & can_load(n_f - 1)
        n_saved = load(early, n_loaded, n_saved)
        n_loaded += early.astype(jnp.int32)

        c = piece(n_b)

        def arrive(n):
            with jax.named_scope("b_wait"):
                local_b(c, n).wait()

                @pl.when(last)
                def _():
                    local_f(c, n).wait()

            with jax.named_scope("b_load"):

                @pl.when(keeps)
                def _():
                    for copy in loads(n_b, c, n):
                        copy.wait()

        late = (do_b == 1) & keeps & (n_loaded == n_b)
        n_saved = load(late, n_loaded, n_saved)
        n_loaded += late.astype(jnp.int32)
        each_size(do_b == 1, c, arrive)
        beside = (do_b == 1) & can_load(n_f - do_f)
        n_saved = load(beside, n_loaded, n_saved)
        n_loaded += beside.astype(jnp.int32)
        each_size(do_b == 1, c, lambda n: take_backward(n_b, c, n))
        n_b += do_b
        behind = (do_b == 1) & can_load(n_f)
        n_saved = load(behind, n_loaded, n_saved)
        n_loaded += behind.astype(jnp.int32)

        @pl.when(do_w == 1)
        def _():
            with jax.named_scope("w"):
                take_weights(n_w)

        return digits, n_f, n_b, n_w + do_w, n_p + do_p, n_saved, n_loaded

    def word(i, carry):
        line, state = carry
        state = lax.fori_loop(i * WORD, i * WORD + WORD, step, (line[0], *state))
        return (*line[1:], line[0]), state[1:]

    lengths = [len(steps(order)) for order in ORDER]
    count = -(-max(lengths) // WORD)
    line = tuple(pick(me, values) for values in zip(*(words(order, count) for order in ORDER), strict=True))
    zero = jnp.int32(0)
    state = lax.fori_loop(0, pick(me, [-(-n // WORD) for n in lengths]), word, (line, (zero,) * 6))[1]
    n_saved = state[4]

    for k in range(CHUNKS - 2, CHUNKS):
        wait_saved(jnp.logical_not(last) & (n_saved <= k), jnp.int32(k))
    for copy, here in ((send_f, last), (send_b, first)):

        @pl.when(jnp.logical_not(here))
        def _(copy=copy):
            for p in range(PIECES - 2 * RING, TAIL_AT, 2):
                copy(p, LARGE).wait_send()
            for p in range(TAIL_AT, PIECES):
                copy(p, SMALL).wait_send()

    if len(OVER_F):
        passed(first, jnp.int32(OVER_F.stop - 1))
    if len(OVER_B):
        passed(last, jnp.int32(OVER_B.stop - 1))

    stores = []
    for j in range(BLOCKS):
        cols = slice(256 * j, 256 * j + 256)
        dgu[0, :, cols] = sum_gu[:, cols].astype(BF16)
        stores.append(pltpu.make_async_copy(dgu.at[0, :, pl.ds(256 * j, 128)], dwg.at[0, :, pl.ds(128 * j, 128)], stored.at[2 * j]))
        stores.append(pltpu.make_async_copy(dgu.at[0, :, pl.ds(256 * j + 128, 128)], dwu.at[0, :, pl.ds(128 * j, 128)], stored.at[2 * j + 1]))
        stores[-2].start()
        stores[-1].start()
    wd[...] = sum_d[...].astype(BF16)
    stores.append(pltpu.make_async_copy(wd, dwd.at[0], stored.at[2 * BLOCKS]))
    stores[-1].start()
    for store in stores:
        store.wait()


def solution(mesh):
    def step(x, dy, w_gate, w_up, w_down):
        v, sem = pltpu.VMEM, pltpu.SemaphoreType.DMA
        return pl.pallas_call(
            kernel,
            out_shape=[jax.ShapeDtypeStruct(w.shape, w.dtype) for w in (w_gate, w_up, w_down)]
            + [jax.ShapeDtypeStruct((MICRO * T, 2 * FF), F32), jax.ShapeDtypeStruct((MICRO * T, FF), BF16)],
            in_specs=[pl.BlockSpec(memory_space=pl.ANY)] * 5,
            out_specs=[pl.BlockSpec(memory_space=pl.ANY)] * 5,
            scratch_shapes=[
                v((MICRO * T, D), BF16), v((DEPTH * T, D), BF16),
                v((D, 2 * FF), BF16), v((FF, D), BF16), v((D, FF), BF16), v((2 * FF, D), BF16),
                v((D, 2 * FF), F32), v((FF, D), F32),
                v((2, LARGE, FF), BF16), v((2, LARGE, 2 * FF), F32), v((2, LARGE, 2 * FF), F32),
                v((SLOTS, T, FF), BF16), v((SLOTS, T, 2 * FF), BF16),
                v((RING * LARGE, D), BF16), v((RING * LARGE, D), BF16),
                sem((PIECES,)), sem((PIECES,)), sem((RING,)), sem((2 * RING,)), sem((2 * RING,)), sem((RING,)),
                sem((4,)), sem((4,)), sem((2 * BLOCKS + 1,)), sem((2 * BLOCKS + 1,)), pltpu.SemaphoreType.REGULAR, pltpu.SemaphoreType.REGULAR,
            ],
            compiler_params=pltpu.CompilerParams(collective_id=0, has_side_effects=True, vmem_limit_bytes=67043328),
        )(x, dy, w_gate, w_up, w_down)[:3]

    return jax.shard_map(
        step,
        mesh=mesh,
        in_specs=(P("rep", None, None),) * 2 + (P("pp", None, None),) * 3,
        out_specs=(P(("rep", "pp"), None, None),) * 3,
        check_vma=False,
    )
```

```python
import jax
import jax.numpy as jnp
from jax import lax
from jax.experimental import pallas as pl
from jax.experimental.pallas import tpu as pltpu
from jax.sharding import PartitionSpec as P

F32, BF16 = jnp.float32, jnp.bfloat16
MESH = pl.DeviceIdType.MESH
MICRO, T, D, FF, STAGES = 16, 512, 512, 1664, 8
LAST = STAGES - 1
BLOCKS = FF // 128
LARGE, SMALL = 256, 128
HEAD, TAIL = 1, 1
RING = 4
SLOTS = 3
DEPTH = 6
OVER_F, OVER_B = range(2, 15), range(1, 13)
ORDER = (
    (0x198911111111111111111, 0x1A1239898191119119111, 0x12224622C2226246A1622, 0x1622262666226226246),
    (0x111111111111111111111, 0x122553331523633331111, 0x122626262626262626266, 0x146222),
    (0x112311111111111111111, 0x126512225751313223111, 0x122626262263625235226, 0x14462222),
    (0x131733131111111111111, 0x123663136225331712711, 0x14622622622626362635),
    (0x153353317331131111111, 0x132523632671233712712, 0x1622662725226251),
    (0x153335325131223111111, 0x171272712312772723513, 0x1462227272522712),
    (0x112535233152311623311, 0x172312527377327377333, 0x14463325233),
    (0x16A26A24C226622226222, 0x14622AE2E2A24EA2A2EE2, 0x14),
)
WORD = 7
INIT_AT = 8

PIECES = MICRO * T // 128
TAIL_AT = PIECES - 4 * TAIL
CHUNKS = 4 * HEAD + 2 * (MICRO - HEAD - TAIL) + 4 * TAIL


def steps(numbers):
    digits = []
    for number in numbers:
        while number > 1:
            digits.append(number % 16)
            number //= 16
    return digits


def words(numbers, count):
    digits = steps(numbers)
    digits += [0] * (WORD * count - len(digits))
    return [sum(d * 16**i for i, d in enumerate(digits[at : at + WORD])) for at in range(0, WORD * count, WORD)]


def piece(k):
    middle, tail = 4 * HEAD, CHUNKS - 4 * TAIL
    return jnp.where(k < middle, k, jnp.where(k < tail, middle + 2 * (k - middle), TAIL_AT + k - tail))


def is_small(p):
    return (p < 4 * HEAD) | (p >= TAIL_AT)


def dot(a, b):
    return jnp.dot(a, b, preferred_element_type=F32)


def dot_rows(a, b):
    return lax.dot_general(a, b, (((0,), (0,)), ((), ())), preferred_element_type=F32)


def sigmoid(x):
    return 0.5 * jnp.tanh(0.5 * x) + 0.5


def scale_of(wide):
    return lax.rsqrt(jnp.mean(wide * wide, -1, keepdims=True) + 1e-6)


def hidden(a, j, wgu):
    both = dot(a, wgu[:, 256 * j : 256 * j + 256])
    gate, up = both[:, :128], both[:, 128:]
    s = sigmoid(gate)
    silu = gate * s
    return silu, up * (s + silu * (1.0 - s)), (silu * up).astype(BF16)


def forward(h, wgu, wd, act, kept):
    wide = h.astype(F32)
    a = (wide * scale_of(wide)).astype(BF16)
    for j in range(BLOCKS):
        silu, slope, act[:, 128 * j : 128 * j + 128] = hidden(a, j, wgu)
        kept[:, 256 * j : 256 * j + 128] = slope
        kept[:, 256 * j + 128 : 256 * j + 256] = silu
    return h + dot(act[...], wd[...]).astype(BF16)


def backward(h, dy, wgu, wdt, wgut, act, dgu, kept, further):
    wide = h.astype(F32)
    scale = scale_of(wide)
    if kept is None:
        a = (wide * scale).astype(BF16)
    for start in range(0, BLOCKS, 2):
        blocks = range(start, min(start + 2, BLOCKS))
        by_act = dot(dy, wdt[:, 128 * start : 128 * blocks[-1] + 128]).astype(BF16).astype(F32)
        for j in blocks:
            by = by_act[:, 128 * (j - start) : 128 * (j - start) + 128]
            if kept is None:
                silu, slope, act[:, 128 * j : 128 * j + 128] = hidden(a, j, wgu)
            else:
                slope, silu = kept[:, 256 * j : 256 * j + 128], kept[:, 256 * j + 128 : 256 * j + 256]
            dgu[:, 256 * j : 256 * j + 128] = (by * slope).astype(BF16)
            dgu[:, 256 * j + 128 : 256 * j + 256] = (by * silu).astype(BF16)
    if not further:
        return None
    by_a = dot(dgu[...], wgut[...]).astype(BF16).astype(F32)
    by_scale = jnp.sum(by_a * wide, -1, keepdims=True)
    by_wide = by_a * scale - wide * (by_scale * scale * scale * scale * (1.0 / D))
    return dy + by_wide.astype(BF16)


def by_weights(h, dy, act, dgu, sum_gu, sum_d):
    wide = h.astype(F32)
    at = (wide * scale_of(wide)).astype(BF16).T
    for start in range(0, FF, 256):
        rows = slice(start, min(start + 256, FF))
        sum_d[rows, :] += dot_rows(act[:, rows], dy).astype(BF16).astype(F32)
    for j in range(BLOCKS):
        at_j = slice(256 * j, 256 * j + 256)
        sum_gu[:, at_j] += dot(at, dgu[:, at_j]).astype(BF16).astype(F32)


def pick(me, values):
    return sum(jnp.where(me == i, v, 0) for i, v in enumerate(values))


def kernel(x, dy, wg_in, wu_in, wd_in, dwg, dwu, dwd, kept_far, act_far, hs, dys, wgu, wgut, sum_gu, sum_d, kept_f, kept_b,
           act, dgu, out_f, out_b, got_f, got_b, got_pass, sent_f, sent_b, sent_pass, saved, loaded, brought, credit, room):
    me = lax.axis_index("pp")
    after, before = lax.rem(me + 1, STAGES), lax.rem(me + LAST, STAGES)
    first, last = me == 0, me == LAST
    wdt, wd, act_f = dwg.at[0], dwd.at[0], dwu.at[0]

    def tokens(ref, p, n):
        return ref.at[p // 4, pl.ds(pl.multiple_of(lax.rem(p, 4) * 128, 128), n), :]

    def rows(p, n):
        return pl.ds(pl.multiple_of(p * 128, 128), n)

    def ring(p, n):
        return rows(lax.rem(p, 2 * RING), n)

    def deep(p, n):
        return rows(lax.rem(p, 4 * DEPTH), n)

    def whole(ref, m):
        return ref.at[rows(lax.rem(m, RING) * 2, LARGE), :]

    fetch = []
    for j in range(BLOCKS):
        fetch.append(pltpu.make_async_copy(wg_in.at[0, :, pl.ds(128 * j, 128)], wgu.at[:, pl.ds(256 * j, 128)], brought.at[2 * j]))
        fetch.append(pltpu.make_async_copy(wu_in.at[0, :, pl.ds(128 * j, 128)], wgu.at[:, pl.ds(256 * j + 128, 128)], brought.at[2 * j + 1]))
    fetch.append(pltpu.make_async_copy(wd_in.at[0], wd, brought.at[2 * BLOCKS]))
    for copy in fetch:
        copy.start()

    def local_f(p, n):
        return pltpu.make_async_copy(tokens(x, p, n), hs.at[rows(p, n), :], got_f.at[p])

    def local_b(p, n):
        return pltpu.make_async_copy(tokens(dy, p, n), dys.at[deep(p, n), :], got_b.at[p])

    def chunks(m):
        n = SMALL if m < HEAD or m >= MICRO - TAIL else LARGE
        return [(4 * m + r // 128, n) for r in range(0, T, n)]

    @pl.when(first)
    def _():
        for m in range(MICRO):
            for chunk in chunks(m):
                local_f(*chunk).start()

    @pl.when(last)
    def _():
        for m in range(DEPTH):
            for chunk in chunks(m):
                local_b(*chunk).start()

    barrier = pltpu.get_barrier_semaphore()
    links = [{i - 1, i + 1} & set(range(STAGES)) for i in range(STAGES)]
    for i, j in ((0, 3), (0, 4), (7, 4), (7, 3)):
        links[i].add(j)
        links[j].add(i)
    for i in range(STAGES):

        @pl.when(me == i)
        def _(i=i):
            for j in sorted(links[i]):
                pl.semaphore_signal(barrier, inc=1, device_id={"pp": j}, device_id_type=MESH)

    pl.semaphore_wait(barrier, pick(me, [len(link) for link in links]))
    for copy in fetch:
        copy.wait()

    def send(source, target, sent, got, device):
        return pltpu.make_async_remote_copy(source, target, sent, got, device_id={"pp": device}, device_id_type=MESH)

    def send_f(p, n):
        return send(out_f.at[ring(p, n), :], hs.at[rows(p, n), :], sent_f.at[lax.rem(p, 2 * RING)], got_f.at[p], after)

    def send_b(p, n):
        return send(out_b.at[ring(p, n), :], dys.at[deep(p, n), :], sent_b.at[lax.rem(p, 2 * RING)], got_b.at[p], before)

    def over_f(p):
        return send(out_f.at[ring(p, LARGE), :], whole(out_b, p // 4), sent_f.at[lax.rem(p, 2 * RING)], got_pass.at[lax.rem(p // 4, RING)], 0)

    def over_b(p):
        return send(out_b.at[ring(p, LARGE), :], whole(out_f, p // 4), sent_b.at[lax.rem(p, 2 * RING)], got_pass.at[lax.rem(p // 4, RING)], LAST)

    def pass_f(m):
        p = 4 * m + 2
        return send(whole(out_b, m), hs.at[rows(p, LARGE), :], sent_pass.at[lax.rem(m, RING)], got_f.at[p], 4)

    def pass_b(m):
        p = 4 * m + 2
        return send(whole(out_f, m), dys.at[deep(p, LARGE), :], sent_pass.at[lax.rem(m, RING)], got_b.at[p], 3)

    def saves(k, p, n):
        buffer = lax.rem(k, 2)
        return (pltpu.make_async_copy(kept_f.at[buffer, pl.ds(0, n), :], kept_far.at[rows(p, n), :], saved.at[2 * buffer]),
                pltpu.make_async_copy(act_f.at[rows(2 * buffer, n), :], act_far.at[rows(p, n), :], saved.at[2 * buffer + 1]))

    def loads(k, p, n):
        buffer, slot, part = lax.rem(k, 2), lax.rem(p // 4, SLOTS), rows(lax.rem(p, 4), n)
        return (pltpu.make_async_copy(kept_far.at[rows(p, n), :], kept_b.at[buffer, pl.ds(0, n), :], loaded.at[2 * buffer]),
                pltpu.make_async_copy(act_far.at[rows(p, n), :], act.at[slot, part, :], loaded.at[2 * buffer + 1]))

    def each_size(condition, p, do):
        for n in (LARGE, SMALL):

            @pl.when(condition & (is_small(p) if n == SMALL else jnp.logical_not(is_small(p))))
            def _(n=n):
                do(n)

    def wait_saved(condition, k):
        p = piece(k)

        def do(n):
            for copy in saves(k, p, n):
                copy.wait()

        @pl.when(condition)
        def _():
            each_size(True, p, do)

    def load(condition, k, have_saved):
        p = piece(k)

        @pl.when(condition)
        def _():
            with jax.named_scope("saved"):
                wait_saved(have_saved <= k, k)

            def do(n):
                for copy in loads(k, p, n):
                    copy.start()

            each_size(True, p, do)

        return jnp.where(condition, jnp.maximum(have_saved, k + 1), have_saved)

    def free_ring(copy, p, n):
        if n == LARGE:

            @pl.when((p >= 2 * RING) & (p < 2 * RING + 4 * HEAD))
            def _():
                copy(p - 2 * RING, SMALL).wait_send()
                copy(p - 2 * RING + 1, SMALL).wait_send()

            @pl.when(p >= 2 * RING + 4 * HEAD)
            def _():
                copy(p - 2 * RING, LARGE).wait_send()
        else:

            @pl.when((p >= TAIL_AT) & (lax.rem(p, 2) == 0))
            def _():
                copy(p - 2 * RING, LARGE).wait_send()

    def inside(m, over):
        return (m >= over.start) & (m < over.stop)

    def passed(condition, m):
        with jax.named_scope("passed"):

            @pl.when(condition)
            def _():
                pass_f(m).wait_send()

            @pl.when(condition & first & inside(m + RING, OVER_F))
            def _():
                pl.semaphore_signal(credit, inc=1, device_id={"pp": 3}, device_id_type=MESH)

            @pl.when(condition & last & inside(m + RING, OVER_B))
            def _():
                pl.semaphore_signal(credit, inc=1, device_id={"pp": 4}, device_id_type=MESH)

    def take_forward(k, p, n, have_saved):
        with jax.named_scope("f_wait"):
            local_f(p, n).wait()
        with jax.named_scope("f_free"):
            free_ring(send_f, p, n)
            wait_saved((k >= 2) & (have_saved <= k - 2), k - 2)
        with jax.named_scope("f"):
            buffer = lax.rem(k, 2)
            out_f[ring(p, n), :] = forward(hs[rows(p, n), :], wgu, wd, act_f.at[rows(2 * buffer, n), :], kept_f.at[buffer, pl.ds(0, n), :])
            via = jnp.bool_(False)
            if n == LARGE and len(OVER_F):
                m = p // 4
                via = (me == 3) & (lax.rem(p, 4) == 2) & inside(m, OVER_F)

                @pl.when(via & (m >= OVER_F.start + RING))
                def _():
                    pl.semaphore_wait(credit, 1)

                @pl.when(via)
                def _():
                    over_f(p).start()

            @pl.when(jnp.logical_not(via))
            def _():
                send_f(p, n).start()

            for copy in saves(k, p, n):
                copy.start()

    def take_backward(k, p, n):
        m, part = p // 4, rows(lax.rem(p, 4), n)
        slot, buffer = lax.rem(m, SLOTS), lax.rem(k, 2)
        act_c, dgu_c, kept = act.at[slot, part, :], dgu.at[slot, part, :], kept_b.at[buffer, pl.ds(0, n), :]
        with jax.named_scope("b"):
            h, by = hs.at[rows(p, n), :], dys.at[deep(p, n), :]

            @pl.when(first)
            def _():
                backward(h[...], by[...], wgu, wdt, wgut, act_c, dgu_c, kept, False)

            @pl.when(jnp.logical_not(first))
            def _():
                @pl.when((m >= DEPTH) & (lax.rem(p, 4) == 0))
                def _():
                    pl.semaphore_wait(room, 1)

                free_ring(send_b, p, n)

            @pl.when(last)
            def _():
                out_b[ring(p, n), :] = backward(h[...], by[...], wgu, wdt, wgut, act_c, dgu_c, None, True)

            @pl.when(jnp.logical_not(first | last))
            def _():
                out_b[ring(p, n), :] = backward(h[...], by[...], wgu, wdt, wgut, act_c, dgu_c, kept, True)

            via = jnp.bool_(False)
            if n == LARGE and len(OVER_B):
                via = (me == 4) & (lax.rem(p, 4) == 2) & inside(m, OVER_B)

                @pl.when(via & (m >= OVER_B.start + RING))
                def _():
                    pl.semaphore_wait(credit, 1)

                @pl.when(via)
                def _():
                    over_b(p).start()

            @pl.when(jnp.logical_not(first | via))
            def _():
                send_b(p, n).start()

    def take_weights(m):
        slot, part = lax.rem(m, SLOTS), pl.ds(pl.multiple_of(m * T, T), T)
        by_weights(hs[part, :], dys[deep(4 * m, T), :], act.at[slot], dgu.at[slot], sum_gu, sum_d)

        @pl.when((m < MICRO - DEPTH) & jnp.logical_not(last))
        def _():
            pl.semaphore_signal(room, inc=1, device_id={"pp": after}, device_id_type=MESH)

        @pl.when(last & (m < MICRO - DEPTH))
        def _():
            for later in range(DEPTH, MICRO):

                @pl.when(m == later - DEPTH)
                def _(later=later):
                    for chunk in chunks(later):
                        local_b(*chunk).start()

    def prepare():
        with jax.named_scope("init"):
            for j in range(BLOCKS):
                wgut[256 * j : 256 * j + 256, :] = wgu[:, 256 * j : 256 * j + 256].T
            for start in range(0, FF, 256):
                at_s = slice(start, min(start + 256, FF))
                wdt[:, at_s] = wd[at_s, :].T
            sum_gu[...] = jnp.zeros_like(sum_gu)
            sum_d[...] = jnp.zeros_like(sum_d)

    def step(s, carry):
        digits, n_f, n_b, n_w, n_p, n_saved, n_loaded = carry
        digit, digits = lax.rem(digits, 16), digits // 16
        do_f, do_b, do_w, do_p = (lax.rem(digit // d, 2) for d in (1, 2, 4, 8))
        keeps = jnp.logical_not(last)

        @pl.when(s == jnp.where(first, INIT_AT, 0))
        def _():
            prepare()

        if len(OVER_F) or len(OVER_B):
            begin = jnp.where(first, OVER_F.start, OVER_B.start)

            @pl.when(do_p == 1)
            def _():
                m = begin + n_p
                passed(n_p > 0, m - 1)
                with jax.named_scope("pass"):
                    pltpu.make_async_copy(tokens(x, 4 * m, LARGE), whole(out_b, m), got_pass.at[lax.rem(m, RING)]).wait()

                    @pl.when(first)
                    def _():
                        pass_f(m).start()

                    @pl.when(last)
                    def _():
                        pass_b(m).start()

        p = piece(n_f)

        @pl.when(do_f == 1)
        def _():
            each_size(True, p, lambda n: take_forward(n_f, p, n, n_saved))

        n_saved = jnp.where((do_f == 1) & (n_f >= 2), jnp.maximum(n_saved, n_f - 1), n_saved)
        n_f += do_f

        def can_load(known):
            return keeps & (n_loaded < known) & (n_loaded < n_b + 2) & (n_w > piece(n_loaded) // 4 - SLOTS)

        early = (do_f == 1) & can_load(n_f - 1)
        n_saved = load(early, n_loaded, n_saved)
        n_loaded += early.astype(jnp.int32)

        c = piece(n_b)

        def arrive(n):
            with jax.named_scope("b_wait"):
                local_b(c, n).wait()

                @pl.when(last)
                def _():
                    local_f(c, n).wait()

            with jax.named_scope("b_load"):

                @pl.when(keeps)
                def _():
                    for copy in loads(n_b, c, n):
                        copy.wait()

        late = (do_b == 1) & keeps & (n_loaded == n_b)
        n_saved = load(late, n_loaded, n_saved)
        n_loaded += late.astype(jnp.int32)

        @pl.when(do_b == 1)
        def _():
            def take(n):
                arrive(n)
                take_backward(n_b, c, n)

            each_size(True, c, take)

        n_b += do_b
        behind = (do_b == 1) & can_load(n_f)
        n_saved = load(behind, n_loaded, n_saved)
        n_loaded += behind.astype(jnp.int32)

        @pl.when(do_w == 1)
        def _():
            with jax.named_scope("w"):
                take_weights(n_w)

        return digits, n_f, n_b, n_w + do_w, n_p + do_p, n_saved, n_loaded

    def word(i, carry):
        line, state = carry
        state = lax.fori_loop(i * WORD, i * WORD + WORD, step, (line[0], *state))
        return (*line[1:], line[0]), state[1:]

    lengths = [len(steps(order)) for order in ORDER]
    count = -(-max(lengths) // WORD)
    line = tuple(pick(me, values) for values in zip(*(words(order, count) for order in ORDER), strict=True))
    zero = jnp.int32(0)
    state = lax.fori_loop(0, pick(me, [-(-n // WORD) for n in lengths]), word, (line, (zero,) * 6))[1]
    n_saved = state[4]

    for k in range(CHUNKS - 2, CHUNKS):
        wait_saved(jnp.logical_not(last) & (n_saved <= k), jnp.int32(k))
    for copy, here in ((send_f, last), (send_b, first)):

        @pl.when(jnp.logical_not(here))
        def _(copy=copy):
            for p in range(PIECES - 2 * RING, TAIL_AT, 2):
                copy(p, LARGE).wait_send()
            for p in range(TAIL_AT, PIECES):
                copy(p, SMALL).wait_send()

    if len(OVER_F):
        passed(first, jnp.int32(OVER_F.stop - 1))
    if len(OVER_B):
        passed(last, jnp.int32(OVER_B.stop - 1))

    for j in range(BLOCKS):
        block = slice(128 * j, 128 * j + 128)
        dwg[0, :, block] = sum_gu[:, 256 * j : 256 * j + 128].astype(BF16)
        dwu[0, :, block] = sum_gu[:, 256 * j + 128 : 256 * j + 256].astype(BF16)
    dwd[0] = sum_d[...].astype(BF16)


def solution(mesh):
    def step(x, dy, w_gate, w_up, w_down):
        v, sem = pltpu.VMEM, pltpu.SemaphoreType.DMA
        return pl.pallas_call(
            kernel,
            out_shape=[pltpu.VMEM(w.shape, w.dtype) for w in (w_gate, w_up, w_down)]
            + [jax.ShapeDtypeStruct((MICRO * T, 2 * FF), F32), jax.ShapeDtypeStruct((MICRO * T, FF), BF16)],
            in_specs=[pl.BlockSpec(memory_space=pl.ANY)] * 5,
            out_specs=[pl.BlockSpec(memory_space=pltpu.VMEM)] * 3 + [pl.BlockSpec(memory_space=pl.ANY)] * 2,
            scratch_shapes=[
                v((MICRO * T, D), BF16), v((DEPTH * T, D), BF16),
                v((D, 2 * FF), BF16), v((2 * FF, D), BF16),
                v((D, 2 * FF), F32), v((FF, D), F32),
                v((2, LARGE, 2 * FF), F32), v((2, LARGE, 2 * FF), F32),
                v((SLOTS, T, FF), BF16), v((SLOTS, T, 2 * FF), BF16),
                v((RING * LARGE, D), BF16), v((RING * LARGE, D), BF16),
                sem((PIECES,)), sem((PIECES,)), sem((RING,)), sem((2 * RING,)), sem((2 * RING,)), sem((RING,)),
                sem((4,)), sem((4,)), sem((2 * BLOCKS + 1,)), pltpu.SemaphoreType.REGULAR, pltpu.SemaphoreType.REGULAR,
            ],
            compiler_params=pltpu.CompilerParams(collective_id=0, has_side_effects=True, vmem_limit_bytes=59 * 2**20 - 2**17),
        )(x, dy, w_gate, w_up, w_down)[:3]

    return jax.shard_map(
        step,
        mesh=mesh,
        in_specs=(P("rep", None, None),) * 2 + (P("pp", None, None),) * 3,
        out_specs=(P(("rep", "pp"), None, None),) * 3,
        check_vma=False,
    )
```

```python
import jax
import jax.numpy as jnp
from jax import lax
from jax.experimental import pallas as pl
from jax.experimental.pallas import tpu as pltpu
from jax.sharding import PartitionSpec as P

F32, BF16 = jnp.float32, jnp.bfloat16
MESH = pl.DeviceIdType.MESH
MICRO, T, D, FF, STAGES = 16, 512, 512, 1664, 8
LAST = STAGES - 1
BLOCKS = FF // 128
LARGE, SMALL = 256, 128
HEAD, TAIL = 1, 1
RING = 4
SLOTS = 3
DEPTH = 6
OVER_F, OVER_B = range(1, 15), range(1, 10)
ORDER = (
    (0x119199911111111111111, 0x12225113991B1A111B991, 0x12622666226266222C82C, 0x1626222666226),
    (0x111111111111111111111, 0x144631332531123113311, 0x162626262626626622632, 0x14622222),
    (0x131331111111111111111, 0x122663515233337251311, 0x122222626262262622653, 0x1446),
    (0x162331111111111111111, 0x125252313631273153131, 0x122222626262622652327, 0x1446),
    (0x171253331231111111111, 0x171733631325272713126, 0x14622262626363253),
    (0x171631631731333111111, 0x125332573337373267313, 0x144622222736),
    (0x165333737731313723131, 0x123271273123167377333, 0x14462335),
    (0x1E62A62C6222462222222, 0x16222622C26AA22C62C2A, 0x146),
)
WORD = 7
INIT_AT = 8

PIECES = MICRO * T // 128
TAIL_AT = PIECES - 4 * TAIL
CHUNKS = 4 * HEAD + 2 * (MICRO - HEAD - TAIL) + 4 * TAIL


def steps(numbers):
    digits = []
    for number in numbers:
        while number > 1:
            digits.append(number % 16)
            number //= 16
    return digits


def words(numbers, count):
    digits = steps(numbers)
    digits += [0] * (WORD * count - len(digits))
    return [sum(d * 16**i for i, d in enumerate(digits[at : at + WORD])) for at in range(0, WORD * count, WORD)]


def piece(k):
    middle, tail = 4 * HEAD, CHUNKS - 4 * TAIL
    return jnp.where(k < middle, k, jnp.where(k < tail, middle + 2 * (k - middle), TAIL_AT + k - tail))


def is_small(p):
    return (p < 4 * HEAD) | (p >= TAIL_AT)


def dot(a, b):
    return jnp.dot(a, b, preferred_element_type=F32)


def dot_rows(a, b):
    return lax.dot_general(a, b, (((0,), (0,)), ((), ())), preferred_element_type=F32)


def sigmoid(x):
    return 0.5 * jnp.tanh(0.5 * x) + 0.5


def scale_of(wide):
    return lax.rsqrt(jnp.mean(wide * wide, -1, keepdims=True) + 1e-6)


def hidden(a, j, wgu):
    both = dot(a, wgu[:, 256 * j : 256 * j + 256])
    gate, up = both[:, :128], both[:, 128:]
    s = sigmoid(gate)
    silu = gate * s
    return silu, up * (s + silu * (1.0 - s)), (silu * up).astype(BF16)


def forward(h, wgu, wd, act, kept):
    wide = h.astype(F32)
    a = (wide * scale_of(wide)).astype(BF16)
    for j in range(BLOCKS):
        silu, slope, act[:, 128 * j : 128 * j + 128] = hidden(a, j, wgu)
        kept[:, 256 * j : 256 * j + 128] = slope
        kept[:, 256 * j + 128 : 256 * j + 256] = silu
    return h + dot(act[...], wd[...]).astype(BF16)


def backward(h, dy, wgu, wdt, wgut, act, dgu, kept, further):
    wide = h.astype(F32)
    scale = scale_of(wide)
    if kept is None:
        a = (wide * scale).astype(BF16)
    for start in range(0, BLOCKS, 2):
        blocks = range(start, min(start + 2, BLOCKS))
        by_act = dot(dy, wdt[:, 128 * start : 128 * blocks[-1] + 128]).astype(BF16).astype(F32)
        for j in blocks:
            by = by_act[:, 128 * (j - start) : 128 * (j - start) + 128]
            if kept is None:
                silu, slope, act[:, 128 * j : 128 * j + 128] = hidden(a, j, wgu)
            else:
                slope, silu = kept[:, 256 * j : 256 * j + 128], kept[:, 256 * j + 128 : 256 * j + 256]
            dgu[:, 256 * j : 256 * j + 128] = (by * slope).astype(BF16)
            dgu[:, 256 * j + 128 : 256 * j + 256] = (by * silu).astype(BF16)
    if not further:
        return None
    by_a = dot(dgu[...], wgut[...]).astype(BF16).astype(F32)
    by_scale = jnp.sum(by_a * wide, -1, keepdims=True)
    by_wide = by_a * scale - wide * (by_scale * scale * scale * scale * (1.0 / D))
    return dy + by_wide.astype(BF16)


def by_weights(h, dy, act, dgu, sum_gu, sum_d):
    wide = h.astype(F32)
    at = (wide * scale_of(wide)).astype(BF16).T
    for start in range(0, FF, 256):
        rows = slice(start, min(start + 256, FF))
        sum_d[rows, :] += dot_rows(act[:, rows], dy).astype(BF16).astype(F32)
    for j in range(BLOCKS):
        at_j = slice(256 * j, 256 * j + 256)
        sum_gu[:, at_j] += dot(at, dgu[:, at_j]).astype(BF16).astype(F32)


def pick(me, values):
    return sum(jnp.where(me == i, v, 0) for i, v in enumerate(values))


def kernel(x, dy, wg_in, wu_in, wd_in, dwg, dwu, dwd, kept_far, act_far, hs, dys, wgu, wgut, sum_gu, sum_d, kept_f, kept_b,
           act, dgu, out_f, out_b, got_f, got_b, got_pass, sent_f, sent_b, sent_pass, saved, loaded, brought, credit, room):
    me = lax.axis_index("pp")
    after, before = lax.rem(me + 1, STAGES), lax.rem(me + LAST, STAGES)
    first, last = me == 0, me == LAST
    wdt, wd, act_f = dwg.at[0], dwd.at[0], dwu.at[0]

    def tokens(ref, p, n):
        return ref.at[p // 4, pl.ds(pl.multiple_of(lax.rem(p, 4) * 128, 128), n), :]

    def rows(p, n):
        return pl.ds(pl.multiple_of(p * 128, 128), n)

    def ring(p, n):
        return rows(lax.rem(p, 2 * RING), n)

    def deep(p, n):
        return rows(lax.rem(p, 4 * DEPTH), n)

    def whole(ref, m):
        return ref.at[rows(lax.rem(m, RING) * 2, LARGE), :]

    fetch = []
    for j in range(BLOCKS):
        fetch.append(pltpu.make_async_copy(wg_in.at[0, :, pl.ds(128 * j, 128)], wgu.at[:, pl.ds(256 * j, 128)], brought.at[2 * j]))
        fetch.append(pltpu.make_async_copy(wu_in.at[0, :, pl.ds(128 * j, 128)], wgu.at[:, pl.ds(256 * j + 128, 128)], brought.at[2 * j + 1]))
    fetch.append(pltpu.make_async_copy(wd_in.at[0], wd, brought.at[2 * BLOCKS]))
    for copy in fetch:
        copy.start()

    def local_f(p, n):
        return pltpu.make_async_copy(tokens(x, p, n), hs.at[rows(p, n), :], got_f.at[p])

    def local_b(p, n):
        return pltpu.make_async_copy(tokens(dy, p, n), dys.at[deep(p, n), :], got_b.at[p])

    def chunks(m):
        n = SMALL if m < HEAD or m >= MICRO - TAIL else LARGE
        return [(4 * m + r // 128, n) for r in range(0, T, n)]

    @pl.when(first)
    def _():
        for m in range(MICRO):
            for chunk in chunks(m):
                local_f(*chunk).start()

    @pl.when(last)
    def _():
        for m in range(DEPTH):
            for chunk in chunks(m):
                local_b(*chunk).start()

    barrier = pltpu.get_barrier_semaphore()
    links = [{i - 1, i + 1} & set(range(STAGES)) for i in range(STAGES)]
    for i, j in ((0, 3), (0, 4), (7, 4), (7, 3)):
        links[i].add(j)
        links[j].add(i)
    for i in range(STAGES):

        @pl.when(me == i)
        def _(i=i):
            for j in sorted(links[i]):
                pl.semaphore_signal(barrier, inc=1, device_id={"pp": j}, device_id_type=MESH)

    pl.semaphore_wait(barrier, pick(me, [len(link) for link in links]))
    for copy in fetch:
        copy.wait()

    def send(source, target, sent, got, device):
        return pltpu.make_async_remote_copy(source, target, sent, got, device_id={"pp": device}, device_id_type=MESH)

    def send_f(p, n):
        return send(out_f.at[ring(p, n), :], hs.at[rows(p, n), :], sent_f.at[lax.rem(p, 2 * RING)], got_f.at[p], after)

    def send_b(p, n):
        return send(out_b.at[ring(p, n), :], dys.at[deep(p, n), :], sent_b.at[lax.rem(p, 2 * RING)], got_b.at[p], before)

    def over_f(p):
        return send(out_f.at[ring(p, LARGE), :], whole(out_b, p // 4), sent_f.at[lax.rem(p, 2 * RING)], got_pass.at[lax.rem(p // 4, RING)], 0)

    def over_b(p):
        return send(out_b.at[ring(p, LARGE), :], whole(out_f, p // 4), sent_b.at[lax.rem(p, 2 * RING)], got_pass.at[lax.rem(p // 4, RING)], LAST)

    def pass_f(m):
        p = 4 * m + 2
        return send(whole(out_b, m), hs.at[rows(p, LARGE), :], sent_pass.at[lax.rem(m, RING)], got_f.at[p], 4)

    def pass_b(m):
        p = 4 * m + 2
        return send(whole(out_f, m), dys.at[deep(p, LARGE), :], sent_pass.at[lax.rem(m, RING)], got_b.at[p], 3)

    def saves(k, p, n):
        buffer = lax.rem(k, 2)
        return (pltpu.make_async_copy(kept_f.at[buffer, pl.ds(0, n), :], kept_far.at[rows(p, n), :], saved.at[2 * buffer]),
                pltpu.make_async_copy(act_f.at[rows(2 * buffer, n), :], act_far.at[rows(p, n), :], saved.at[2 * buffer + 1]))

    def loads(k, p, n):
        buffer, slot, part = lax.rem(k, 2), lax.rem(p // 4, SLOTS), rows(lax.rem(p, 4), n)
        return (pltpu.make_async_copy(kept_far.at[rows(p, n), :], kept_b.at[buffer, pl.ds(0, n), :], loaded.at[2 * buffer]),
                pltpu.make_async_copy(act_far.at[rows(p, n), :], act.at[slot, part, :], loaded.at[2 * buffer + 1]))

    def each_size(condition, p, do):
        for n in (LARGE, SMALL):

            @pl.when(condition & (is_small(p) if n == SMALL else jnp.logical_not(is_small(p))))
            def _(n=n):
                do(n)

    def wait_saved(condition, k):
        p = piece(k)

        def do(n):
            for copy in saves(k, p, n):
                copy.wait()

        @pl.when(condition)
        def _():
            each_size(True, p, do)

    def load(condition, k, have_saved):
        p = piece(k)

        @pl.when(condition)
        def _():
            with jax.named_scope("saved"):
                wait_saved(have_saved <= k, k)

            def do(n):
                for copy in loads(k, p, n):
                    copy.start()

            each_size(True, p, do)

        return jnp.where(condition, jnp.maximum(have_saved, k + 1), have_saved)

    def free_ring(copy, p, n):
        if n == LARGE:

            @pl.when((p >= 2 * RING) & (p < 2 * RING + 4 * HEAD))
            def _():
                copy(p - 2 * RING, SMALL).wait_send()
                copy(p - 2 * RING + 1, SMALL).wait_send()

            @pl.when(p >= 2 * RING + 4 * HEAD)
            def _():
                copy(p - 2 * RING, LARGE).wait_send()
        else:

            @pl.when((p >= TAIL_AT) & (lax.rem(p, 2) == 0))
            def _():
                copy(p - 2 * RING, LARGE).wait_send()

    def inside(m, over):
        return (m >= over.start) & (m < over.stop)

    def passed(condition, m):
        with jax.named_scope("passed"):

            @pl.when(condition)
            def _():
                pass_f(m).wait_send()

            @pl.when(condition & first & inside(m + RING, OVER_F))
            def _():
                pl.semaphore_signal(credit, inc=1, device_id={"pp": 3}, device_id_type=MESH)

            @pl.when(condition & last & inside(m + RING, OVER_B))
            def _():
                pl.semaphore_signal(credit, inc=1, device_id={"pp": 4}, device_id_type=MESH)

    def take_forward(k, p, n, have_saved):
        with jax.named_scope("f_wait"):
            local_f(p, n).wait()
        with jax.named_scope("f_free"):
            free_ring(send_f, p, n)
            wait_saved((k >= 2) & (have_saved <= k - 2), k - 2)
        with jax.named_scope("f"):
            buffer = lax.rem(k, 2)
            out_f[ring(p, n), :] = forward(hs[rows(p, n), :], wgu, wd, act_f.at[rows(2 * buffer, n), :], kept_f.at[buffer, pl.ds(0, n), :])
            via = jnp.bool_(False)
            if n == LARGE and len(OVER_F):
                m = p // 4
                via = (me == 3) & (lax.rem(p, 4) == 2) & inside(m, OVER_F)

                @pl.when(via & (m >= OVER_F.start + RING))
                def _():
                    pl.semaphore_wait(credit, 1)

                @pl.when(via)
                def _():
                    over_f(p).start()

            @pl.when(jnp.logical_not(via))
            def _():
                send_f(p, n).start()

            for copy in saves(k, p, n):
                copy.start()

    def take_backward(k, p, n):
        m, part = p // 4, rows(lax.rem(p, 4), n)
        slot, buffer = lax.rem(m, SLOTS), lax.rem(k, 2)
        act_c, dgu_c, kept = act.at[slot, part, :], dgu.at[slot, part, :], kept_b.at[buffer, pl.ds(0, n), :]
        with jax.named_scope("b"):
            h, by = hs.at[rows(p, n), :], dys.at[deep(p, n), :]

            @pl.when(first)
            def _():
                backward(h[...], by[...], wgu, wdt, wgut, act_c, dgu_c, kept, False)

            @pl.when(jnp.logical_not(first))
            def _():
                @pl.when((m >= DEPTH) & (lax.rem(p, 4) == 0))
                def _():
                    pl.semaphore_wait(room, 1)

                free_ring(send_b, p, n)

            @pl.when(last)
            def _():
                out_b[ring(p, n), :] = backward(h[...], by[...], wgu, wdt, wgut, act_c, dgu_c, None, True)

            @pl.when(jnp.logical_not(first | last))
            def _():
                out_b[ring(p, n), :] = backward(h[...], by[...], wgu, wdt, wgut, act_c, dgu_c, kept, True)

            via = jnp.bool_(False)
            if n == LARGE and len(OVER_B):
                via = (me == 4) & (lax.rem(p, 4) == 2) & inside(m, OVER_B)

                @pl.when(via & (m >= OVER_B.start + RING))
                def _():
                    pl.semaphore_wait(credit, 1)

                @pl.when(via)
                def _():
                    over_b(p).start()

            @pl.when(jnp.logical_not(first | via))
            def _():
                send_b(p, n).start()

    def take_weights(m):
        slot, part = lax.rem(m, SLOTS), pl.ds(pl.multiple_of(m * T, T), T)
        by_weights(hs[part, :], dys[deep(4 * m, T), :], act.at[slot], dgu.at[slot], sum_gu, sum_d)

        @pl.when((m < MICRO - DEPTH) & jnp.logical_not(last))
        def _():
            pl.semaphore_signal(room, inc=1, device_id={"pp": after}, device_id_type=MESH)

        @pl.when(last & (m < MICRO - DEPTH))
        def _():
            for later in range(DEPTH, MICRO):

                @pl.when(m == later - DEPTH)
                def _(later=later):
                    for chunk in chunks(later):
                        local_b(*chunk).start()

    def prepare():
        with jax.named_scope("init"):
            for j in range(BLOCKS):
                wgut[256 * j : 256 * j + 256, :] = wgu[:, 256 * j : 256 * j + 256].T
            for start in range(0, FF, 256):
                at_s = slice(start, min(start + 256, FF))
                wdt[:, at_s] = wd[at_s, :].T
            sum_gu[...] = jnp.zeros_like(sum_gu)
            sum_d[...] = jnp.zeros_like(sum_d)

    def step(s, carry):
        digits, n_f, n_b, n_w, n_p, n_saved, n_loaded = carry
        digit, digits = lax.rem(digits, 16), digits // 16
        do_f, do_b, do_w, do_p = (lax.rem(digit // d, 2) for d in (1, 2, 4, 8))
        keeps = jnp.logical_not(last)

        @pl.when(s == jnp.where(first, INIT_AT, 0))
        def _():
            prepare()

        if len(OVER_F) or len(OVER_B):
            begin = jnp.where(first, OVER_F.start, OVER_B.start)

            @pl.when(do_p == 1)
            def _():
                m = begin + n_p
                passed(n_p > 0, m - 1)
                with jax.named_scope("pass"):
                    pltpu.make_async_copy(tokens(x, 4 * m, LARGE), whole(out_b, m), got_pass.at[lax.rem(m, RING)]).wait()

                    @pl.when(first)
                    def _():
                        pass_f(m).start()

                    @pl.when(last)
                    def _():
                        pass_b(m).start()

        p = piece(n_f)

        @pl.when(do_f == 1)
        def _():
            each_size(True, p, lambda n: take_forward(n_f, p, n, n_saved))

        n_saved = jnp.where((do_f == 1) & (n_f >= 2), jnp.maximum(n_saved, n_f - 1), n_saved)
        n_f += do_f

        def can_load(known):
            return keeps & (n_loaded < known) & (n_loaded < n_b + 2) & (n_w > piece(n_loaded) // 4 - SLOTS)

        early = (do_f == 1) & can_load(n_f - 1)
        n_saved = load(early, n_loaded, n_saved)
        n_loaded += early.astype(jnp.int32)

        c = piece(n_b)

        def arrive(n):
            with jax.named_scope("b_wait"):
                local_b(c, n).wait()

                @pl.when(last)
                def _():
                    local_f(c, n).wait()

            with jax.named_scope("b_load"):

                @pl.when(keeps)
                def _():
                    for copy in loads(n_b, c, n):
                        copy.wait()

        late = (do_b == 1) & keeps & (n_loaded == n_b)
        n_saved = load(late, n_loaded, n_saved)
        n_loaded += late.astype(jnp.int32)

        @pl.when(do_b == 1)
        def _():
            def take(n):
                arrive(n)
                take_backward(n_b, c, n)

            each_size(True, c, take)

        n_b += do_b
        behind = (do_b == 1) & can_load(n_f)
        n_saved = load(behind, n_loaded, n_saved)
        n_loaded += behind.astype(jnp.int32)

        @pl.when(do_w == 1)
        def _():
            with jax.named_scope("w"):
                take_weights(n_w)

        return digits, n_f, n_b, n_w + do_w, n_p + do_p, n_saved, n_loaded

    def word(i, carry):
        line, state = carry
        state = lax.fori_loop(i * WORD, i * WORD + WORD, step, (line[0], *state))
        return (*line[1:], line[0]), state[1:]

    lengths = [len(steps(order)) for order in ORDER]
    count = -(-max(lengths) // WORD)
    line = tuple(pick(me, values) for values in zip(*(words(order, count) for order in ORDER), strict=True))
    zero = jnp.int32(0)
    state = lax.fori_loop(0, pick(me, [-(-n // WORD) for n in lengths]), word, (line, (zero,) * 6))[1]
    n_saved = state[4]

    for k in range(CHUNKS - 2, CHUNKS):
        wait_saved(jnp.logical_not(last) & (n_saved <= k), jnp.int32(k))
    for copy, here in ((send_f, last), (send_b, first)):

        @pl.when(jnp.logical_not(here))
        def _(copy=copy):
            for p in range(PIECES - 2 * RING, TAIL_AT, 2):
                copy(p, LARGE).wait_send()
            for p in range(TAIL_AT, PIECES):
                copy(p, SMALL).wait_send()

    if len(OVER_F):
        passed(first, jnp.int32(OVER_F.stop - 1))
    if len(OVER_B):
        passed(last, jnp.int32(OVER_B.stop - 1))

    for j in range(BLOCKS):
        block = slice(128 * j, 128 * j + 128)
        dwg[0, :, block] = sum_gu[:, 256 * j : 256 * j + 128].astype(BF16)
        dwu[0, :, block] = sum_gu[:, 256 * j + 128 : 256 * j + 256].astype(BF16)
    dwd[0] = sum_d[...].astype(BF16)


def solution(mesh):
    def step(x, dy, w_gate, w_up, w_down):
        v, sem = pltpu.VMEM, pltpu.SemaphoreType.DMA
        return pl.pallas_call(
            kernel,
            out_shape=[pltpu.VMEM(w.shape, w.dtype) for w in (w_gate, w_up, w_down)]
            + [jax.ShapeDtypeStruct((MICRO * T, 2 * FF), F32), jax.ShapeDtypeStruct((MICRO * T, FF), BF16)],
            in_specs=[pl.BlockSpec(memory_space=pl.ANY)] * 5,
            out_specs=[pl.BlockSpec(memory_space=pltpu.VMEM)] * 3 + [pl.BlockSpec(memory_space=pl.ANY)] * 2,
            scratch_shapes=[
                v((MICRO * T, D), BF16), v((DEPTH * T, D), BF16),
                v((D, 2 * FF), BF16), v((2 * FF, D), BF16),
                v((D, 2 * FF), F32), v((FF, D), F32),
                v((2, LARGE, 2 * FF), F32), v((2, LARGE, 2 * FF), F32),
                v((SLOTS, T, FF), BF16), v((SLOTS, T, 2 * FF), BF16),
                v((RING * LARGE, D), BF16), v((RING * LARGE, D), BF16),
                sem((PIECES,)), sem((PIECES,)), sem((RING,)), sem((2 * RING,)), sem((2 * RING,)), sem((RING,)),
                sem((4,)), sem((4,)), sem((2 * BLOCKS + 1,)), pltpu.SemaphoreType.REGULAR, pltpu.SemaphoreType.REGULAR,
            ],
            compiler_params=pltpu.CompilerParams(collective_id=0, has_side_effects=True, vmem_limit_bytes=59 * 2**20 - 2**17),
        )(x, dy, w_gate, w_up, w_down)[:3]

    return jax.shard_map(
        step,
        mesh=mesh,
        in_specs=(P("rep", None, None),) * 2 + (P("pp", None, None),) * 3,
        out_specs=(P(("rep", "pp"), None, None),) * 3,
        check_vma=False,
    )
```
